768 devices in a mesh: wide: 96 (over z, x, core), tile: 8 (over y).
Axes of the slice: x: 4, y: 8, z: 12, core: 2. Of those that a mesh axis runs over, the one named last changes fastest.
Arguments:
- interface_gaps: float32 [96, 8, 2, 192, 256], P('wide', 'tile'), may hold values from -50 to 50
- flexibility: bfloat16 [96, 8, 768, 768], P('wide', 'tile'), may hold values from -1 to 2, as said below
- dirichlet_schur: bfloat16 [96, 8, 768, 768], P('wide', 'tile'), may hold values from -1 to 2, as said below
- face_rows: int32 [96, 8, 4], P('wide', 'tile'), may hold values from 0 to 192, as said below
Outputs:
- multipliers: float32 [96, 8, 2, 192, 256], P('wide', 'tile')
- residual: float32 [96, 8, 2, 192, 256], P('wide', 'tile')
The draws below stay inside these ranges and needn't reach their ends.
Inputs may be any that keep to these rules, and one draw needn't show every extreme that they name: `face_rows`: A subdomain's previous-face counts equal its neighbour's next-face counts; faces on the boundary of the grid have 0 rows, every other face 192 // 2 rows or more; some face has exactly 192 rows. `flexibility`: each subdomain's matrix is symmetric positive definite. `dirichlet_schur`: each subdomain's matrix is symmetric positive definite.
All inputs are finite; a program needn't handle non-finite values.
Results may differ from the reference program's by a relative error of at most 0.009.
The reference program's roundings to bfloat16 on the way count: a program that leaves them out, or rounds other values in their place, can miss the bound.
Values may be sent and summed in bfloat16 or wider, within the bound.
No kernel may reach another device: no remote copies, remote signals or barrier semaphores. Data moves between devices by JAX's collectives and lax.ppermute only.
A program may use at most 32 MiB of HBM per device.

```python
import math
import jax
import jax.numpy as jnp
from jax import lax

FACE = 192
ROWS = 768
LOADS = 256
ITERS = 3
GRID_W = 96
GRID_T = 8


def draw_face_rows(key, part):
    first_key, second_key = jax.random.split(jax.random.fold_in(key, 11))
    next_wide = jax.random.randint(first_key, (GRID_W, GRID_T), FACE // 2, FACE + 1).astype(jnp.int32)
    next_wide = next_wide.at[0, 0].set(FACE)
    next_wide = jnp.where((jnp.arange(GRID_W) < GRID_W - 1)[:, None], next_wide, 0).astype(jnp.int32)
    next_tile = jax.random.randint(second_key, (GRID_W, GRID_T), FACE // 2, FACE + 1).astype(jnp.int32)
    next_tile = next_tile.at[0, 0].set(FACE)
    next_tile = jnp.where((jnp.arange(GRID_T) < GRID_T - 1)[None, :], next_tile, 0).astype(jnp.int32)
    prev_wide = jnp.concatenate([jnp.zeros((1, GRID_T), jnp.int32), next_wide[:-1]], 0)
    prev_tile = jnp.concatenate([jnp.zeros((GRID_W, 1), jnp.int32), next_tile[:, :-1]], 1)
    return jnp.stack([next_wide, next_tile, prev_wide, prev_tile], -1)


def operator_matrices(key):
    identity = jnp.eye(ROWS, dtype=jnp.float32)

    def single(index):
        sub_key = jax.random.fold_in(key, index)
        entry_key, diagonal_key = jax.random.split(sub_key)
        raw_entries = jax.random.uniform(entry_key, (ROWS, ROWS), jnp.float32, -1.0, 1.0)
        symmetric = (raw_entries + raw_entries.T) * (0.37 / math.sqrt(ROWS))
        diagonal_part = jax.random.uniform(diagonal_key, (ROWS,), jnp.float32, 1.0, 2.0)
        matrix = symmetric * (1.0 - identity) + identity * diagonal_part[:, None]
        return matrix.astype(jnp.bfloat16)
    return lax.map(single, jnp.arange(GRID_W * GRID_T)).reshape(GRID_W, GRID_T, ROWS, ROWS)


def draw_flexibility(key, part):
    return operator_matrices(jax.random.fold_in(key, 23))


def draw_dirichlet_schur(key, part):
    return operator_matrices(jax.random.fold_in(key, 37))


def draw_interface_gaps(key, part):
    base_key, column_key, rough_key = jax.random.split(jax.random.fold_in(key, 51), 3)
    shape = (GRID_W, GRID_T, 2, FACE, LOADS)
    wide_scale = (0.5 + jnp.arange(GRID_W, dtype=jnp.float32) / (GRID_W - 1)).reshape(GRID_W, 1, 1, 1, 1)
    column_scale = jnp.exp(jax.random.uniform(column_key, (LOADS,), jnp.float32, math.log(0.3), math.log(3.0)))
    rough = jax.random.uniform(rough_key, (GRID_W, GRID_T, 2, FACE, 1), jnp.float32, 0.5, 2.0)
    base = jnp.clip(jax.random.normal(base_key, shape, jnp.float32), -4.0, 4.0)
    return base * rough * column_scale * wide_scale


def setup_inputs(seed: int = 0) -> dict:
    seeds = jax.random.split(jax.random.key(seed), 5)
    return {
        "interface_gaps": draw_interface_gaps(jax.random.fold_in(seeds[4], 71), 0),
        "flexibility": draw_flexibility(jax.random.fold_in(seeds[4], 71), 0),
        "dirichlet_schur": draw_dirichlet_schur(jax.random.fold_in(seeds[4], 71), 0),
        "face_rows": draw_face_rows(jax.random.fold_in(seeds[4], 71), 0),
    }


def face_masks(face_rows):
    row_index = jnp.arange(FACE, dtype=jnp.int32)
    return (row_index[None, None, None, :, None] < face_rows[:, :, :, None, None]).astype(jnp.float32)


def lift_faces(owned_vec):
    next_wide = owned_vec[:, :, 0]
    next_tile = owned_vec[:, :, 1]
    below_wide = jnp.concatenate([jnp.zeros_like(next_wide[:1]), next_wide[:-1]], 0)
    below_tile = jnp.concatenate([jnp.zeros_like(next_tile[:, :1]), next_tile[:, :-1]], 1)
    local_vec = jnp.stack([next_wide, next_tile, -below_wide, -below_tile], 2)
    return local_vec.astype(jnp.bfloat16).reshape(GRID_W, GRID_T, 4 * FACE, LOADS)


def apply_blocks(matrices, local_vec):
    def single(stacked):
        matrix, lifted = stacked
        return jnp.einsum("jrc,jck->jrk", matrix.astype(jnp.float32), lifted.astype(jnp.float32),
                          precision=lax.Precision.HIGHEST)
    return lax.map(single, (matrices, local_vec))


def assemble(result, face_mask):
    faces = result.reshape(GRID_W, GRID_T, 4, FACE, LOADS)
    above_wide = jnp.concatenate([faces[1:, :, 2], jnp.zeros_like(faces[:1, :, 2])], 0)
    above_tile = jnp.concatenate([faces[:, 1:, 3], jnp.zeros_like(faces[:, :1, 3])], 1)
    return jnp.stack([faces[:, :, 0] - above_wide, faces[:, :, 1] - above_tile], 2) * face_mask[:, :, :2]


def operate(matrices, owned_vec, face_mask):
    return assemble(apply_blocks(matrices, lift_faces(owned_vec)), face_mask)


def column_dots(left, right):
    return jnp.sum(left * right, axis=(0, 1, 2, 3))


def reference(interface_gaps, flexibility, dirichlet_schur, face_rows):
    face_mask = face_masks(face_rows)
    residual = interface_gaps * face_mask[:, :, :2]
    multipliers = jnp.zeros_like(residual)
    precond = operate(dirichlet_schur, residual, face_mask)
    mapped = operate(flexibility, precond, face_mask)
    gamma_now = column_dots(residual, precond)
    curvature = column_dots(precond, mapped)
    step_len = gamma_now / curvature
    direction = precond
    along_dir = mapped
    for iteration in range(ITERS):
        multipliers = multipliers + step_len * direction
        residual = residual - step_len * along_dir
        if iteration + 1 < ITERS:
            precond = operate(dirichlet_schur, residual, face_mask)
            mapped = operate(flexibility, precond, face_mask)
            gamma_next = column_dots(residual, precond)
            curvature = column_dots(precond, mapped)
            scaling = gamma_next / gamma_now
            step_len = gamma_next / (curvature - scaling * gamma_next / step_len)
            direction = precond + scaling * direction
            along_dir = mapped + scaling * along_dir
            gamma_now = gamma_next
    return multipliers, residual
```

```python
import functools
import jax
import jax.numpy as jnp
from jax import lax
from jax.experimental import pallas as pl
from jax.experimental.pallas import tpu as pltpu
from jax.sharding import Mesh, PartitionSpec as P

ITERS = 3
CHUNK = 32
F32, BF16 = jnp.float32, jnp.bfloat16
VMEM = pl.BlockSpec(memory_space=pltpu.VMEM)
SMEM = pl.BlockSpec(memory_space=pltpu.SMEM)
WIDE = ("z", "x", "core")


def shifted(block, axis, distance):
    size = lax.axis_size(axis)
    route = [(i - distance, i) for i in range(size) if 0 <= i - distance < size]
    return lax.ppermute(block, axis, route)


def exchange(faces):
    below_tile = shifted(faces[1], "y", 1)
    above_tile = shifted(faces[3], "y", -1)
    below_wide = shifted(faces[0], WIDE, 1)
    above_wide = shifted(faces[2], WIDE, -1)
    return above_wide, above_tile, below_wide, below_tile


def pieces(rows):
    return [slice(start, start + CHUNK) for start in range(0, rows, CHUNK)]


def row_mask(start, count, columns):
    index = lax.broadcasted_iota(jnp.int32, (CHUNK, columns), 0) + start
    return index < count


def folded(block):
    return jnp.sum(block.reshape(block.shape[0] // 8, 8, block.shape[1]), axis=0)


def multiply(matrix_ref, lifted_ref, vector_at, faces, product_ref):
    rows, columns = faces[0].shape
    product_ref[...] = jnp.dot(matrix_ref[...], lifted_ref[...], preferred_element_type=F32)
    totals = [jnp.zeros((8, columns), F32), jnp.zeros((8, columns), F32)]
    for face in range(4):
        for piece in pieces(rows):
            whole = slice(face * rows + piece.start, face * rows + piece.stop)
            value = product_ref[whole, :]
            faces[face][piece, :] = value
            totals[face // 2] += folded(vector_at(face, piece) * value)
    return jnp.sum(totals[0] - totals[1], axis=0, keepdims=True)


def first_kernel(counts, matrix, gaps, below_wide, below_tile, res, gamma, f0, f1, f2, f3, lifted, product):
    rows, columns = below_wide.shape
    for face in range(4):
        for piece in pieces(rows):
            if face < 2:
                value = gaps[face, piece, :]
            else:
                value = (below_wide, below_tile)[face - 2][piece, :]
            value = jnp.where(row_mask(piece.start, counts[face], columns), value, 0.0)
            res[face, piece, :] = value
            signed = value if face < 2 else -value
            lifted[face * rows + piece.start : face * rows + piece.stop, :] = signed.astype(BF16)
    gamma[...] = multiply(matrix, lifted, lambda f, p: res[f, p, :], (f0, f1, f2, f3), product)


def assembled(face, piece, own, across, count):
    value = own[face][piece, :] - across[face][piece, :]
    if face >= 2:
        value = -value
    return jnp.where(row_mask(piece.start, count, value.shape[1]), value, 0.0)


def flex_kernel(counts, matrix, y0, y1, y2, y3, a0, a1, b0, b1, gamma, pre, sums, f0, f1, f2, f3, lifted, product):
    rows, columns = y0.shape
    own, across = (y0, y1, y2, y3), (a0, a1, b0, b1)
    for face in range(4):
        for piece in pieces(rows):
            value = assembled(face, piece, own, across, counts[face])
            pre[face, piece, :] = value
            signed = value if face < 2 else -value
            lifted[face * rows + piece.start : face * rows + piece.stop, :] = signed.astype(BF16)
    sums[0:1, :] = gamma[...]
    sums[1:2, :] = multiply(matrix, lifted, lambda f, p: pre[f, p, :], (f0, f1, f2, f3), product)


def step_sizes(first, sums, scal):
    gamma, curvature = sums[0:1, :], sums[1:2, :]
    if first:
        return gamma, gamma / curvature, None
    scaling = gamma / scal[0:1, :]
    return gamma, gamma / (curvature - scaling * gamma / scal[1:2, :]), scaling


def update_kernel(first, *refs):
    (counts, matrix, sums, y0, y1, y2, y3, a0, a1, b0, b1, pre, res), refs = refs[:13], refs[13:]
    if not first:
        (scal, direction, along, mult), refs = refs[:4], refs[4:]
    res_out, direction_out, along_out, mult_out, scal_out, gamma_out, f0, f1, f2, f3, lifted, product = refs
    rows, columns = y0.shape
    gamma, step, scaling = step_sizes(first, sums, None if first else scal)
    scal_out[0:1, :] = gamma
    scal_out[1:2, :] = step
    own, across = (y0, y1, y2, y3), (a0, a1, b0, b1)
    for face in range(4):
        for piece in pieces(rows):
            mapped = assembled(face, piece, own, across, counts[face])
            if not first:
                mapped = mapped + scaling * along[face, piece, :]
            along_out[face, piece, :] = mapped
            value = res[face, piece, :] - step * mapped
            res_out[face, piece, :] = value
            signed = value if face < 2 else -value
            lifted[face * rows + piece.start : face * rows + piece.stop, :] = signed.astype(BF16)
            if face < 2:
                way = pre[face, piece, :]
                if not first:
                    way = way + scaling * direction[face, piece, :]
                direction_out[face, piece, :] = way
                moved = step * way
                mult_out[face, piece, :] = moved if first else mult[face, piece, :] + moved
    gamma_out[...] = multiply(matrix, lifted, lambda f, p: res_out[f, p, :], (f0, f1, f2, f3), product)


def last_kernel(counts, sums, y0, y1, a0, a1, pre, res, scal, direction, along, mult, mult_out, res_out):
    rows, columns = y0.shape
    gamma, step, scaling = step_sizes(False, sums, scal)
    for face in range(2):
        for piece in pieces(rows):
            mapped = assembled(face, piece, (y0, y1), (a0, a1), counts[face])
            mapped = mapped + scaling * along[face, piece, :]
            res_out[face, piece, :] = res[face, piece, :] - step * mapped
            way = pre[face, piece, :] + scaling * direction[face, piece, :]
            mult_out[face, piece, :] = mult[face, piece, :] + step * way


def call(kernel, outs, args, name, size=None):
    scratch = []
    flops = 0
    if size is not None:
        rows, columns = size
        scratch = [pltpu.VMEM((rows, columns), BF16), pltpu.VMEM((rows, columns), F32)]
        flops = 2 * rows * rows * columns
    moved = sum(a.size * a.dtype.itemsize for a in args) + 4 * sum(o.size for o in outs)
    return pl.pallas_call(
        kernel,
        out_shape=outs,
        in_specs=[SMEM] + [VMEM] * (len(args) - 1),
        out_specs=[VMEM] * len(outs),
        scratch_shapes=scratch,
        name=name,
        cost_estimate=pl.CostEstimate(flops=flops, bytes_accessed=moved, transcendentals=0),
        compiler_params=pltpu.CompilerParams(vmem_limit_bytes=24 * 1024 * 1024),
    )(*args)


def total(sums, stages):
    for axes in stages:
        sums = lax.optimization_barrier(lax.psum(sums, axes))
    return sums


STAGES = (
    ("y", "z", ("x", "core")),
    ("y", "z", "x", "core"),
    (("core", "y"), "x", "z"),
)


def per_device(interface_gaps, flexibility, dirichlet_schur, face_rows):
    rows, columns = interface_gaps.shape[3:]
    counts = face_rows[0, 0]
    flex, schur = flexibility[0, 0], dirichlet_schur[0, 0]
    gaps = interface_gaps[0, 0]
    size = (4 * rows, columns)
    four = jax.ShapeDtypeStruct((4, rows, columns), F32)
    two = jax.ShapeDtypeStruct((2, rows, columns), F32)
    face = jax.ShapeDtypeStruct((rows, columns), F32)
    line = jax.ShapeDtypeStruct((1, columns), F32)
    pair = jax.ShapeDtypeStruct((2, columns), F32)
    faces = [face] * 4

    below_tile = shifted(gaps[1], "y", 1)
    below_wide = shifted(gaps[0], WIDE, 1)
    res, gamma, *out = call(
        first_kernel, [four, line] + faces, [counts, schur, gaps, below_wide, below_tile], "first", size
    )
    state = []
    for iteration in range(ITERS):
        across = exchange(out)
        pre, sums, *out = call(
            flex_kernel, [four, pair] + faces, [counts, flex, *out, *across, gamma], "flex", size
        )
        if iteration + 1 < ITERS:
            across = exchange(out)
            sums = total(sums, STAGES[iteration])
            res, direction, along, mult, scal, gamma, *out = call(
                functools.partial(update_kernel, iteration == 0),
                [four, two, four, two, pair, line] + faces,
                [counts, schur, sums, *out, *across, pre, res, *state],
                "update",
                size,
            )
            state = [scal, direction, along, mult]
        else:
            above_tile = shifted(out[3], "y", -1)
            above_wide = shifted(out[2], WIDE, -1)
            sums = total(sums, STAGES[iteration])
            mult, res = call(
                last_kernel, [two, two], [counts, sums, out[0], out[1], above_wide, above_tile, pre, res, *state], "last"
            )
    return mult[None, None], res[None, None]


def solution(mesh):
    wide, tile = mesh.devices.shape
    split = Mesh(mesh.devices.reshape(wide // 8, 4, 2, tile), ("z", "x", "core", "y"))
    placed = (
        P(WIDE, "y", None, None, None),
        P(WIDE, "y", None, None),
        P(WIDE, "y", None, None),
        P(WIDE, "y", None),
    )
    return jax.shard_map(
        per_device,
        mesh=split,
        in_specs=placed,
        out_specs=(P(WIDE, "y", None, None, None), P(WIDE, "y", None, None, None)),
        check_vma=False,
    )
```

```python
import functools
import jax
import jax.numpy as jnp
from jax import lax
from jax.experimental import pallas as pl
from jax.experimental.pallas import tpu as pltpu
from jax.sharding import Mesh, PartitionSpec as P

ITERS = 3
CHUNK = 32
F32, BF16 = jnp.float32, jnp.bfloat16
VMEM = pl.BlockSpec(memory_space=pltpu.VMEM)
SMEM = pl.BlockSpec(memory_space=pltpu.SMEM)
WIDE = ("z", "x", "core")


def shifted(block, axis, distance):
    size = lax.axis_size(axis)
    route = [(i - distance, i) for i in range(size) if 0 <= i - distance < size]
    return lax.ppermute(block, axis, route)


def exchange(faces):
    below_tile = shifted(faces[1], "y", 1)
    above_tile = shifted(faces[3], "y", -1)
    below_wide = shifted(faces[0], WIDE, 1)
    above_wide = shifted(faces[2], WIDE, -1)
    return above_wide, above_tile, below_wide, below_tile


def pieces(rows):
    return [slice(start, start + CHUNK) for start in range(0, rows, CHUNK)]


def row_mask(start, count, columns):
    index = lax.broadcasted_iota(jnp.int32, (CHUNK, columns), 0) + start
    return index < count


def folded(block):
    return jnp.sum(block.reshape(block.shape[0] // 8, 8, block.shape[1]), axis=0)


def multiply(matrix_ref, lifted_ref, vector_at, faces, product_ref):
    rows, columns = faces[0].shape
    product_ref[...] = jnp.dot(matrix_ref[...], lifted_ref[...], preferred_element_type=F32)
    totals = [jnp.zeros((8, columns), F32), jnp.zeros((8, columns), F32)]
    for face in range(4):
        for piece in pieces(rows):
            whole = slice(face * rows + piece.start, face * rows + piece.stop)
            value = product_ref[whole, :]
            faces[face][piece, :] = value
            totals[face // 2] += folded(vector_at(face, piece) * value)
    return jnp.sum(totals[0] - totals[1], axis=0, keepdims=True)


def first_kernel(counts, matrix, gaps, below_wide, below_tile, res, gamma, f0, f1, f2, f3, lifted, product, behind):
    rows, columns = below_wide.shape
    for face in range(4):
        for piece in pieces(rows):
            if face < 2:
                value = gaps[face, piece, :]
            else:
                value = (below_wide, below_tile)[face - 2][piece, :]
            value = jnp.where(row_mask(piece.start, counts[face], columns), value, 0.0)
            res[face, piece, :] = value
            signed = value if face < 2 else -value
            lifted[face * rows + piece.start : face * rows + piece.stop, :] = signed.astype(BF16)
    gamma[...] = multiply(matrix, lifted, lambda f, p: res[f, p, :], (f0, f1, f2, f3), product)


def assembled(face, piece, own, across, count):
    value = own[face][piece, :] - across[face][piece, :]
    if face >= 2:
        value = -value
    return jnp.where(row_mask(piece.start, count, value.shape[1]), value, 0.0)


def flex_kernel(counts, matrix, y0, y1, y2, y3, a0, a1, b0, b1, gamma, pre, sums, f0, f1, f2, f3, lifted, product, behind):
    rows, columns = y0.shape
    own, across = (y0, y1, y2, y3), (a0, a1, b0, b1)

    def place(face):
        return (pre, face) if face < 2 else (behind, face - 2)

    for face in range(4):
        held, slot = place(face)
        for piece in pieces(rows):
            value = assembled(face, piece, own, across, counts[face])
            held[slot, piece, :] = value
            signed = value if face < 2 else -value
            lifted[face * rows + piece.start : face * rows + piece.stop, :] = signed.astype(BF16)

    def vector_at(face, piece):
        held, slot = place(face)
        return held[slot, piece, :]

    curvature = multiply(matrix, lifted, vector_at, (f0, f1, f2, f3), product)
    copies = sums.shape[0]
    sums[:, 0:1, :] = jnp.broadcast_to(gamma[...][None], (copies, 1, columns))
    sums[:, 1:2, :] = jnp.broadcast_to(curvature[None], (copies, 1, columns))


def step_sizes(sums, scal):
    gathered = jnp.sum(sums[...], axis=0)
    gamma, curvature = gathered[0:1], gathered[1:2]
    if scal is None:
        return gamma, gamma / curvature, None
    scaling = gamma / scal[0:1, :]
    return gamma, gamma / (curvature - scaling * gamma / scal[1:2, :]), scaling


def update_kernel(first, *refs):
    (counts, matrix, sums, y0, y1, y2, y3, a0, a1, b0, b1, res), refs = refs[:12], refs[12:]
    scal = along = None
    if not first:
        (scal, along), refs = refs[:2], refs[2:]
    res_out, along_out, scal_out, gamma_out, f0, f1, f2, f3, lifted, product, behind = refs
    rows, columns = y0.shape
    gamma, step, scaling = step_sizes(sums, scal)
    scal_out[0:1, :] = gamma
    scal_out[1:2, :] = step
    scal_out[2:3, :] = step if first else scal[1:2, :]
    scal_out[3:4, :] = jnp.zeros_like(step) if first else scaling
    own, across = (y0, y1, y2, y3), (a0, a1, b0, b1)
    for face in range(4):
        for piece in pieces(rows):
            mapped = assembled(face, piece, own, across, counts[face])
            if not first:
                mapped = mapped + scaling * along[face, piece, :]
            along_out[face, piece, :] = mapped
            value = res[face, piece, :] - step * mapped
            res_out[face, piece, :] = value
            signed = value if face < 2 else -value
            lifted[face * rows + piece.start : face * rows + piece.stop, :] = signed.astype(BF16)
    gamma_out[...] = multiply(matrix, lifted, lambda f, p: res_out[f, p, :], (f0, f1, f2, f3), product)


def last_kernel(counts, sums, y0, y1, a0, a1, res, scal, along, pre0, pre1, pre2, mult_out, res_out):
    rows, columns = y0.shape
    _, step2, scaling2 = step_sizes(sums, scal)
    step1, step0, scaling1 = scal[1:2, :], scal[2:3, :], scal[3:4, :]
    weight2 = step2
    weight1 = step1 + step2 * scaling2
    weight0 = step0 + weight1 * scaling1
    for face in range(2):
        for piece in pieces(rows):
            mapped = assembled(face, piece, (y0, y1), (a0, a1), counts[face])
            mapped = mapped + scaling2 * along[face, piece, :]
            res_out[face, piece, :] = res[face, piece, :] - step2 * mapped
            mult_out[face, piece, :] = (
                weight0 * pre0[face, piece, :] + weight1 * pre1[face, piece, :] + weight2 * pre2[face, piece, :]
            )


def call(kernel, outs, args, name, size=None):
    scratch = []
    flops = 0
    if size is not None:
        rows, columns = size
        scratch = [pltpu.VMEM((rows, columns), BF16), pltpu.VMEM((rows, columns), F32)]
        scratch += [pltpu.VMEM((2, rows // 4, columns), F32)]
        flops = 2 * rows * rows * columns
    moved = sum(a.size * a.dtype.itemsize for a in args) + 4 * sum(o.size for o in outs)
    return pl.pallas_call(
        kernel,
        out_shape=outs,
        in_specs=[SMEM] + [VMEM] * (len(args) - 1),
        out_specs=[VMEM] * len(outs),
        scratch_shapes=scratch,
        name=name,
        cost_estimate=pl.CostEstimate(flops=flops, bytes_accessed=moved, transcendentals=0),
        compiler_params=pltpu.CompilerParams(vmem_limit_bytes=24 * 1024 * 1024),
    )(*args)


def relay_kernel(held, out):
    out[...] = jnp.broadcast_to(jnp.sum(held[...], axis=0, keepdims=True), out.shape)


def split_kernel(gaps, wide, tile):
    wide[...] = gaps[0]
    tile[...] = gaps[1]


def small_call(kernel, outs, arg, name):
    return pl.pallas_call(
        kernel,
        out_shape=outs,
        in_specs=[VMEM],
        out_specs=[VMEM] * len(outs),
        name=name,
        compiler_params=pltpu.CompilerParams(vmem_limit_bytes=4 * 1024 * 1024),
    )(arg)


def gathered(sums, stages):
    for index, axes in enumerate(stages):
        if index:
            out = jax.ShapeDtypeStruct((lax.axis_size(axes), *sums.shape[1:]), F32)
            (sums,) = small_call(relay_kernel, [out], sums, "relay")
        sums = lax.all_to_all(sums, axes, 0, 0)
    return sums


STAGES = (
    ("y", "z", ("x", "core")),
    (("core", "y"), ("z", "x")),
    (("x", "core", "y"), "z"),
)


def per_device(interface_gaps, flexibility, dirichlet_schur, face_rows):
    rows, columns = interface_gaps.shape[3:]
    counts = face_rows[0, 0]
    flex, schur = flexibility[0, 0], dirichlet_schur[0, 0]
    gaps = interface_gaps[0, 0]
    size = (4 * rows, columns)
    four = jax.ShapeDtypeStruct((4, rows, columns), F32)
    two = jax.ShapeDtypeStruct((2, rows, columns), F32)
    face = jax.ShapeDtypeStruct((rows, columns), F32)
    line = jax.ShapeDtypeStruct((1, columns), F32)
    scalars = jax.ShapeDtypeStruct((4, columns), F32)
    faces = [face] * 4

    wide_gaps, tile_gaps = small_call(split_kernel, [face, face], gaps, "split")
    below_tile = shifted(tile_gaps, "y", 1)
    below_wide = shifted(wide_gaps, WIDE, 1)
    res, gamma, *out = call(
        first_kernel, [four, line] + faces, [counts, schur, gaps, below_wide, below_tile], "first", size
    )
    state, pres = [], []
    for iteration in range(ITERS):
        stages = STAGES[iteration]
        partial = jax.ShapeDtypeStruct((lax.axis_size(stages[0]), 2, columns), F32)
        across = exchange(out)
        pre, sums, *out = call(
            flex_kernel, [two, partial] + faces, [counts, flex, *out, *across, gamma], "flex", size
        )
        pres.append(pre)
        if iteration + 1 < ITERS:
            across = exchange(out)
            sums = gathered(sums, stages)
            res, along, scal, gamma, *out = call(
                functools.partial(update_kernel, iteration == 0),
                [four, four, scalars, line] + faces,
                [counts, schur, sums, *out, *across, res, *state],
                "update",
                size,
            )
            state = [scal, along]
        else:
            above_tile = shifted(out[3], "y", -1)
            above_wide = shifted(out[2], WIDE, -1)
            sums = gathered(sums, stages)
            mult, res = call(
                last_kernel, [two, two], [counts, sums, out[0], out[1], above_wide, above_tile, res, *state, *pres], "last"
            )
    return mult[None, None], res[None, None]


def solution(mesh):
    wide, tile = mesh.devices.shape
    split = Mesh(mesh.devices.reshape(wide // 8, 4, 2, tile), ("z", "x", "core", "y"))
    placed = (
        P(WIDE, "y", None, None, None),
        P(WIDE, "y", None, None),
        P(WIDE, "y", None, None),
        P(WIDE, "y", None),
    )
    return jax.shard_map(
        per_device,
        mesh=split,
        in_specs=placed,
        out_specs=(P(WIDE, "y", None, None, None), P(WIDE, "y", None, None, None)),
        check_vma=False,
    )
```
